256 devices in a mesh: grp: 16 (over y, z_lo, core), sp: 16 (over z_hi, x).
Axes of the slice: x: 4, y: 4, z: 8 (z_hi: 4, z_lo: 2; z = z_hi * 2 + z_lo), core: 2. Of those that a mesh axis runs over, the one named last changes fastest.
Arguments:
- bucket_of: int32 [16], replicated, may hold values from 0 to 3, as said below
- lengths: int32 [4], replicated, may hold values from 256 to 1024, as said below
- counts: int32 [4], replicated, may hold values from 256 to 4096
- queries: bfloat16 [32768, 4096], P(('grp', 'sp')), may hold values from -4.5 to 4.5
- keys: bfloat16 [32768, 4096], P(('grp', 'sp')), may hold values from -4.5 to 4.5
- values: bfloat16 [32768, 4096], P(('grp', 'sp')), may hold values from -6 to 6
- out_grad: bfloat16 [32768, 3072], P(('grp', 'sp')), may hold values from -24 to 24
- w_out: bfloat16 [4096, 3072], P('sp', 'grp'), may hold values from -1.75 to 1.75
Outputs:
- grad_queries: bfloat16 [32768, 4096], P(('grp', 'sp'))
- grad_keys: bfloat16 [32768, 4096], P(('grp', 'sp'))
- grad_values: bfloat16 [32768, 4096], P(('grp', 'sp'))
- grad_w_out: float32 [4096, 3072], P('sp', 'grp')
The draws below stay inside these ranges and needn't reach their ends.
Inputs may be any that keep to these rules, and one draw needn't show every extreme that they name: `bucket_of`: every one of the 4 buckets is held by at least one group. `lengths`: one bucket has length exactly 1024.
All inputs are finite; a program needn't handle non-finite values.
Results may differ from the reference program's by a relative error of at most 0.0091.
Values may be sent and summed in bfloat16 or wider, within the bound.
A program may use at most 128 MiB of HBM per device.

```python
from functools import partial
import jax
import jax.numpy as jnp
from jax import lax

D = 3072
HEAD_DIM = 128
SEQS = 2
NB = 4
GROUPS = 16
GTOK = 2048
CAP = 1024
HD = 4096
TOKENS = 32768


def shared_pattern(key):
    pattern_key = jax.random.fold_in(key, 404)
    signs = jnp.where(jax.random.bernoulli(jax.random.fold_in(pattern_key, 1), 0.5, (HD,)), 4.5, -4.5)
    query_spot = jax.random.randint(jax.random.fold_in(pattern_key, 2), (), 0, CAP)
    key_spot = jax.random.randint(jax.random.fold_in(pattern_key, 3), (), 0, max(CAP // 4, 1))
    return (signs, query_spot, key_spot)


def draw_queries(key, part):
    signs, query_spot, key_spot = shared_pattern(key)
    own_key = jax.random.fold_in(key, 11)
    filled = jnp.clip(jax.random.normal(own_key, (TOKENS, HD)), -4.5, 4.5)
    return filled.astype(jnp.bfloat16)


def draw_keys(key, part):
    signs, query_spot, key_spot = shared_pattern(key)
    own_key = jax.random.fold_in(key, 12)
    filled = jnp.clip(jax.random.normal(own_key, (TOKENS, HD)), -4.5, 4.5)
    return filled.astype(jnp.bfloat16)


def draw_bucket_of(key, part):
    first = jax.random.permutation(jax.random.fold_in(key, 21), NB).astype(jnp.int32)
    others = jax.random.randint(jax.random.fold_in(key, 22), (GROUPS,), 0, NB).astype(jnp.int32)
    listed = jnp.concatenate([first, others])[:GROUPS]
    return jax.random.permutation(jax.random.fold_in(key, 23), listed).astype(jnp.int32)


def draw_lengths(key, part):
    drawn = jax.random.randint(jax.random.fold_in(key, 31), (NB,), CAP // 4, CAP + 1)
    longest = jax.random.randint(jax.random.fold_in(key, 32), (), 0, NB)
    return jnp.where(jnp.arange(NB) == longest, CAP, drawn).astype(jnp.int32)


def touch_ends(array, stream_key, least, largest):
    extent = array.shape
    place = [jax.random.randint(jax.random.fold_in(stream_key, axis), (), 0, extent[axis]) for axis in range(len(extent))]
    array = array.at[tuple(place)].set(least)
    longest = extent.index(max(extent))
    place[longest] = (place[longest] + 1) % extent[longest]
    return array.at[tuple(place)].set(largest)


def spiked(array, stream_key, source, target, shards_of, factor):
    owner, partner = [(jnp.arange(array.shape[axis_at]) // (array.shape[axis_at] // shards_of)).reshape([-1 if axis == axis_at else 1 for axis in range(array.ndim)]) for axis_at in (source, target)]
    chosen = jax.random.permutation(stream_key, shards_of)[partner]
    strong = (owner == chosen) | (owner == (partner + shards_of // 2) % shards_of)
    return jnp.where(strong, factor * array, array)


def level_of(key, dims, split, least, top_value):
    gain, own = 1.0, jax.random.fold_in(key, 6)
    for position, parts in split:
        draws = jnp.exp(jax.random.uniform(jax.random.fold_in(own, position), (parts,), jnp.float32, least / len(split), top_value / len(split)))
        gain = gain * jnp.repeat(draws, dims[position] // parts).reshape([-1 if axis == position else 1 for axis in range(len(dims))])
    return gain


def centred(key, shape, scale, most, split=(), held_as=jnp.bfloat16):
    gain = level_of(key, shape, split, -0.22, 0.18) if split else 1.0
    values = jax.random.normal(key, shape, jnp.float32) * scale * gain
    return jnp.minimum(jnp.maximum(values, -most), most).astype(held_as)


def heavy_noise(stream_key, dims, spread, limit, shards, heavy, kind=jnp.bfloat16):
    result = spread * jax.random.normal(stream_key, dims, jnp.float32)
    if shards:
        result = result * level_of(stream_key, dims, shards, -0.22, 0.18)
    return jnp.clip(spiked(result, jax.random.fold_in(stream_key, 3), *heavy), -limit, limit).astype(kind)


def setup_inputs(seed: int = 0) -> dict:
    splits = jax.random.split(jax.random.key(seed), 9)
    bucket_of = draw_bucket_of(jax.random.fold_in(splits[8], 71), 0)
    lengths = draw_lengths(jax.random.fold_in(splits[8], 71), 0)
    counts = touch_ends(jax.random.randint(splits[2], (NB,), 256, 4097), jax.random.fold_in(splits[2], 1), 256, 4096).astype(jnp.int32)
    queries = draw_queries(jax.random.fold_in(splits[8], 71), 0)
    keys = draw_keys(jax.random.fold_in(splits[8], 71), 0)
    values = centred(splits[5], (TOKENS, HD), 1.0, 6.0, ((0, 256),))
    out_grad = heavy_noise(splits[6], (TOKENS, D), 1.0, 24.0, ((0, 256),), (0, 1, 256, 6.0))
    w_out = centred(splits[7], (HD, D), (max(D // 256, 1)) ** -0.5, 1.75, ((0, 16), (1, 16)))
    return dict(bucket_of=bucket_of, lengths=lengths, counts=counts, queries=queries, keys=keys, values=values, out_grad=out_grad, w_out=w_out)


def dot_nt(first_op, second_op):
    return lax.dot_general(first_op, second_op, (((1,), (1,)), ((), ())), preferred_element_type=jnp.float32)


def dot_tn(first_op, second_op):
    return lax.dot_general(first_op, second_op, (((0,), (0,)), ((), ())), preferred_element_type=jnp.float32)


def probabilities(query_rows, key_rows, keep_cols):
    scores = dot_nt(query_rows, key_rows) * (query_rows.shape[1] ** -0.5)
    scores = jnp.where(keep_cols[None, :], scores, -jnp.inf)
    row_top = jnp.max(scores, axis=1, keepdims=True)
    row_exp = jnp.exp(scores - row_top)
    return row_exp / jnp.sum(row_exp, axis=1, keepdims=True)


def item_grads(operands, keep_cols):
    query_rows, key_rows, value_rows, d_item = operands
    probs_full = probabilities(query_rows, key_rows, keep_cols)
    probs_low = probs_full.astype(jnp.bfloat16)
    attn_item = jnp.dot(probs_low, value_rows, preferred_element_type=jnp.float32).astype(jnp.bfloat16)
    row_delta = jnp.sum(d_item.astype(jnp.float32) * attn_item.astype(jnp.float32), axis=1, keepdims=True)
    dscore = (probs_full * (dot_nt(d_item, value_rows) - row_delta)).astype(jnp.bfloat16)
    factor = query_rows.shape[1] ** -0.5
    grad_q = (jnp.dot(dscore, key_rows, preferred_element_type=jnp.float32) * factor).astype(jnp.bfloat16)
    grad_k = (dot_tn(dscore, query_rows) * factor).astype(jnp.bfloat16)
    grad_v = dot_tn(probs_low, d_item).astype(jnp.bfloat16)
    return attn_item, grad_q, grad_k, grad_v


def split_heads(stacked, head_count):
    return stacked.reshape(SEQS, CAP, head_count, HEAD_DIM).transpose(0, 2, 1, 3).reshape(SEQS * head_count, CAP, HEAD_DIM)


def join_heads(stacked, head_count):
    return stacked.reshape(SEQS, head_count, CAP, HEAD_DIM).transpose(0, 2, 1, 3).reshape(SEQS * CAP, head_count * HEAD_DIM)


def reference(bucket_of, lengths, counts, queries, keys, values, out_grad, w_out):
    head_count = w_out.shape[0] // HEAD_DIM
    group_counts = counts[bucket_of].astype(jnp.float32)
    weights = group_counts / jnp.sum(group_counts)
    group_lengths = lengths[bucket_of]

    def one_group(running, group_index):
        row_first = (group_index * GTOK).astype(jnp.int32)
        slices = [lax.dynamic_slice_in_dim(source, row_first, GTOK, 0) for source in (queries, keys, values, out_grad)]
        keep_cols = jnp.arange(CAP, dtype=jnp.int32) < group_lengths[group_index]
        keep_rows = jnp.tile(keep_cols, SEQS)
        d_full = dot_nt(slices[3], w_out)
        d_attn = (d_full * keep_rows[:, None].astype(jnp.float32)).astype(jnp.bfloat16)
        operands = tuple(split_heads(source, head_count) for source in (slices[0], slices[1], slices[2], d_attn))
        attn_heads, grad_q, grad_k, grad_v = lax.map(partial(item_grads, keep_cols=keep_cols), operands)
        masked = join_heads(attn_heads, head_count) * keep_rows[:, None].astype(jnp.bfloat16)
        grad_part = dot_tn(masked, slices[3])
        return running + weights[group_index] * grad_part, (join_heads(grad_q, head_count), join_heads(grad_k, head_count), join_heads(grad_v, head_count))

    start_grad = jnp.zeros((w_out.shape[0], w_out.shape[1]), jnp.float32)
    summed_grad, stacked_grads = lax.scan(one_group, start_grad, jnp.arange(GROUPS, dtype=jnp.int32))
    grad_q, grad_k, grad_v = stacked_grads
    width = grad_q.shape[2]
    return grad_q.reshape(TOKENS, width), grad_k.reshape(TOKENS, width), grad_v.reshape(TOKENS, width), summed_grad
```

```python
import jax
import jax.numpy as jnp
from jax import lax
from jax.experimental import pallas as pl
from jax.experimental.pallas import tpu as pltpu
from jax.sharding import PartitionSpec as P

MESH = pl.DeviceIdType.MESH
BF = jnp.bfloat16
F32 = jnp.float32
LOG2E = 1.4426950408889634
SCALE = 128 ** (-0.5)
NEG = -1e30
QT = 256


def dot_nn(a, b):
    return lax.dot_general(a, b, (((1,), (0,)), ((), ())), preferred_element_type=F32)


def dot_nt(a, b):
    return lax.dot_general(a, b, (((1,), (1,)), ((), ())), preferred_element_type=F32)


def kernel(
    bucket_ref, len_ref, cnt_ref, q_in, k_in, v_in, g_in, w_in,
    dq_out, dk_out, dv_out, gw_out,
    qb, kb, vb, kt, vt, gb, wb, do_t, pn, o_t, at_own, at_oth,
    w_own, w_got, bias, st_own, st_got, st_fin, ds,
    dq_own, dq_send, dq_got, dq_fin, dk_fin, dv_fin,
    gw_send, gw_got, gy_send, gy_got, gz, gz_got, fin_send, fin_got,
    s_loc, s_qkv, r_qkv, s_q2, r_q2, s_gz, r_gz, s_gx, r_gx, s_w, r_wc, r_wz, r_wy, r_wd,
    s_st, s_dq, r_dq, s_out, r_out, s_gc, r_gc, s_gy, r_gy, s_gzz, r_gzz, s_fin,
):
    g = lax.axis_index("grp")
    s = lax.axis_index("sp")
    core = lax.rem(g, 2)
    zl = lax.rem(lax.div(g, 2), 2)
    y = lax.div(g, 4)
    x = lax.rem(s, 4)
    zh = lax.div(s, 4)
    half = lax.rem(zh, 2)
    z = zh * 2 + zl

    def dev(x_=None, zh_=None, y_=None, zl_=None, core_=None):
        x_ = x if x_ is None else x_
        zh_ = zh if zh_ is None else zh_
        y_ = y if y_ is None else y_
        zl_ = zl if zl_ is None else zl_
        core_ = core if core_ is None else core_
        return {"grp": y_ * 4 + zl_ * 2 + core_, "sp": zh_ * 4 + x_}

    def zdev(z_):
        return dev(zh_=lax.div(z_, 2), zl_=lax.rem(z_, 2))

    def xs_of(d):
        return lax.rem(x + d, 4)

    def ys_of(d):
        return lax.rem(y + d, 4)

    def zs_of(d):
        return lax.rem(z + d, 8)

    other = dev(core_=1 - core)
    mate_zh = zh + 1 - 2 * half
    mate = dev(zh_=mate_zh)

    def m(v, k):
        return pl.multiple_of(v, k)

    sends = []

    def send(src, dst, ss, rs, device):
        c = pltpu.make_async_remote_copy(
            src_ref=src, dst_ref=dst, send_sem=ss, recv_sem=rs, device_id=device, device_id_type=MESH
        )
        c.start()
        return c

    def got(ref, sem):
        pltpu.make_async_copy(ref, ref, sem).wait()

    barrier = pltpu.get_barrier_semaphore()
    peers = [dev(x_=xs_of(d)) for d in (1, 2, 3)]
    peers += [dev(y_=ys_of(d)) for d in (1, 2, 3)]
    peers += [zdev(zs_of(d)) for d in range(1, 8)]
    peers += [other]
    for p in peers:
        pl.semaphore_signal(barrier, inc=1, device_id=p, device_id_type=MESH)
    pl.semaphore_wait(barrier, len(peers))

    seq_len = len_ref[bucket_ref[g]]
    total = cnt_ref[bucket_ref[0]]
    for i in range(1, 16):
        total = total + cnt_ref[bucket_ref[i]]
    weight = cnt_ref[bucket_ref[g]].astype(F32) / total.astype(F32)

    row_me = half * 512 + x * 128
    loc = []

    def local(src, dst, i):
        c = pltpu.make_async_copy(src, dst, s_loc.at[i])
        c.start()
        loc.append(c)
        return c

    for i in range(4):
        sends.append(send(
            g_in.at[pl.ds(i * 32, 32), :], gb.at[pl.ds(m(row_me + i * 32, 32), 32), :],
            s_gz.at[i], r_gz.at[i], mate))
    sends.append(send(
        w_in.at[pl.ds(m((1 - core) * 128, 128), 128), :], w_got, s_w.at[0], r_wc, other))
    lw = local(w_in.at[pl.ds(m(core * 128, 128), 128), :], w_own, 0)

    def blocks(src, dst, row, xp, a):
        out = []
        for b in range(4):
            out.append((src.at[:, pl.ds(m((b * 4 + xp) * 256, 256), 256)],
                        dst.at[pl.ds(row, 128), pl.ds(b * 256, 256)]))
        return out

    arrs = ((q_in, qb, m(row_me, 128)), (k_in, kb, m(x * 128, 128)), (v_in, vb, m(x * 128, 128)))

    def send_x(a):
        src, dst, row = arrs[a]
        for d in (1, 3, 2):
            xp = xs_of(d)
            for sr, dr in blocks(src, dst, row, xp, a):
                send(sr, dr, s_qkv.at[a * 4 + d], r_qkv.at[a, x], dev(x_=xp))

    for a in range(3):
        src, dst, row = arrs[a]
        for b, (sr, dr) in enumerate(blocks(src, dst, row, x, a)):
            local(sr, dr, 1 + a * 4 + b)
    lg = local(g_in, gb.at[pl.ds(m(row_me, 128), 128), :], 13)

    left, right = dev(x_=xs_of(3)), dev(x_=xs_of(1))

    def g_rows(hh, xs, i):
        return gb.at[pl.ds(m(hh * 512 + xs * 128 + i * 32, 32), 32), :]

    send_x(0)
    for i in range(4):
        for j, p in enumerate((right, left)):
            sends.append(send(
                g_in.at[pl.ds(i * 32, 32), :], g_rows(half, x, i),
                s_gx.at[i * 2 + j], r_gx.at[0, x, i], p))
    send_x(1)
    send_x(2)

    lw.wait()
    got(w_got, r_wc)
    r_i = lax.broadcasted_iota(jnp.int32, (192, 384), 0)
    c_i = lax.broadcasted_iota(jnp.int32, (192, 384), 1)
    e_own = jnp.where(c_i == r_i + core * 192, 1.0, 0.0).astype(BF)
    e_oth = jnp.where(c_i == r_i + (1 - core) * 192, 1.0, 0.0).astype(BF)

    def w_blk(zz):
        return wb.at[pl.ds(m(lax.div(zz, 2) * 256 + core * 128, 128), 128),
                     pl.ds(m((y * 2 + lax.rem(zz, 2)) * 384, 128), 384)]

    w_blk(z)[...] = (dot_nn(w_own[...], e_own) + dot_nn(w_got[...], e_oth)).astype(BF)
    for d in (4, 3, 5, 2, 6, 1, 7):
        sends.append(send(w_blk(z), w_blk(z), s_w.at[d], r_wz.at[z], zdev(zs_of(d))))

    for c in loc[1:5]:
        c.wait()

    def q_rows(hh, xs):
        return qb.at[pl.ds(m(hh * 512 + xs * 128, 128), 128), :]

    sends.append(send(q_rows(half, x), q_rows(half, x), s_q2.at[0], r_q2.at[x], mate))
    for d in (1, 3, 2):
        xs = xs_of(d)
        got(q_rows(half, xs), r_qkv.at[0, xs])
        sends.append(send(q_rows(half, xs), q_rows(half, xs), s_q2.at[d], r_q2.at[xs], mate))

    xr = xs_of(1)

    def w_row(ys, b):
        return wb.at[pl.ds(m(b * 256 + core * 128, 128), 128), pl.ds(m(ys * 768, 128), 768)]

    for i in range(4):
        got(g_rows(half, xr, i), r_gx.at[0, xr, i])
        sends.append(send(g_rows(half, xr, i), g_rows(half, xr, i), s_gx.at[8 + i], r_gx.at[0, xr, i], left))
        if i == 0:
            for d in range(1, 8):
                zz = zs_of(d)
                got(w_blk(zz), r_wz.at[zz])
            for b in range(4):
                for d in (2, 1, 3):
                    sends.append(send(w_row(y, b), w_row(y, b), s_w.at[8 + b * 4 + d], r_wy.at[y, b], dev(y_=ys_of(d))))
            for b in range(4):
                sends.append(send(w_row(y, b), w_row(y, b), s_w.at[8 + b * 4], r_wd.at[y, b], other))
        oh = 1 - half
        got(g_rows(oh, x, i), r_gz.at[i])
        for j, p in enumerate((right, left)):
            sends.append(send(g_rows(oh, x, i), g_rows(oh, x, i), s_gx.at[12 + i * 2 + j], r_gx.at[1, x, i], p))

    for c in loc[5:]:
        c.wait()
    for a, buf in ((1, kb), (2, vb)):
        for d in (1, 3, 2):
            xs = xs_of(d)
            got(buf.at[pl.ds(m(xs * 128, 128), 128), :], r_qkv.at[a, xs])

    key_pos = lax.broadcasted_iota(jnp.int32, (512, QT), 0) + half * 512
    bias[...] = jnp.where(key_pos < seq_len, 0.0, NEG)

    def col(h):
        return pl.ds(m(h * 128, 128), 128)

    def flip(h, c):
        kt[col(h), :] = kb[:, col(h)].T
        vt[col(h), :] = vb[:, col(h)].T
        return c

    lax.fori_loop(0, 8, flip, 0)

    def forward(q0):
        def body(h, c):
            sc = dot_nt(kb[:, col(h)], qb[pl.ds(q0, QT), col(h)])
            sc = sc * (SCALE * LOG2E) + bias[...]
            top = jnp.max(sc, axis=0, keepdims=True)
            pe = jnp.exp2(sc - top)
            st_own[pl.ds(h, 1), pl.ds(q0, QT)] = top
            st_own[pl.ds(8 + h, 1), pl.ds(q0, QT)] = jnp.sum(pe, axis=0, keepdims=True)
            pb = pe.astype(BF)
            pn[h, :, pl.ds(q0, QT)] = pb
            o_t[col(h), pl.ds(q0, QT)] = dot_nn(vt[col(h), :], pb)
            return c

        lax.fori_loop(0, 8, body, 0)

    own0 = m(half * 512, 256)
    oth0 = m((1 - half) * 512, 256)
    for t in range(2):
        forward(m(own0 + t * QT, 256))

    for d in (1, 3, 2):
        ys = ys_of(d)
        for b in range(4):
            got(w_row(ys, b), r_wy.at[ys, b])
            sends.append(send(w_row(ys, b), w_row(ys, b), s_w.at[24 + d * 4 + b], r_wd.at[ys, b], other))

    oh = 1 - half
    for i in range(4):
        got(g_rows(oh, xr, i), r_gx.at[1, xr, i])
        sends.append(send(g_rows(oh, xr, i), g_rows(oh, xr, i), s_gx.at[20 + i], r_gx.at[1, xr, i], left))

    def w_row_oth(ys, b):
        return wb.at[pl.ds(m(b * 256 + (1 - core) * 128, 128), 128), pl.ds(m(ys * 768, 128), 768)]

    for d in range(4):
        ys = ys_of(d)
        for b in range(4):
            got(w_row_oth(ys, b), r_wd.at[ys, b])

    for d in (2, 3):
        xs = xs_of(d)
        for i in range(4):
            got(g_rows(half, xs, i), r_gx.at[0, xs, i])

    def grads(q0):
        def body(i, c):
            rows = pl.ds(m(i * 256, 256), 256)
            do_t[rows, pl.ds(q0, 256)] = dot_nt(wb[rows, :], gb[pl.ds(q0, 256), :]).astype(BF)
            return c

        lax.fori_loop(0, 4, body, 0)

    for t in range(2):
        grads(m(own0 + t * 256, 256))

    for d in range(4):
        xs = xs_of(d)
        got(q_rows(oh, xs), r_q2.at[xs])
    for t in range(2):
        forward(m(oth0 + t * QT, 256))

    for d in (2, 3):
        xs = xs_of(d)
        for i in range(4):
            got(g_rows(oh, xs, i), r_gx.at[1, xs, i])
    for t in range(2):
        grads(m(oth0 + t * 256, 256))

    def delta(h, c):
        st_own[pl.ds(16 + h, 1), :] = jnp.sum(
            do_t[col(h), :].astype(F32) * o_t[col(h), :], axis=0, keepdims=True)
        return c

    lax.fori_loop(0, 8, delta, 0)
    sends.append(send(st_own, st_got, s_st.at[0], s_st.at[1], mate))
    got(st_got, s_st.at[1])

    top_own, top_got = st_own[pl.ds(0, 8), :], st_got[pl.ds(0, 8), :]
    top = jnp.maximum(top_own, top_got)
    a_own, a_got = jnp.exp2(top_own - top), jnp.exp2(top_got - top)
    length = st_own[pl.ds(8, 8), :] * a_own + st_got[pl.ds(8, 8), :] * a_got
    dsum = (st_own[pl.ds(16, 8), :] * a_own + st_got[pl.ds(16, 8), :] * a_got) / length
    q_pos = lax.rem(lax.broadcasted_iota(jnp.int32, (8, 1024), 1), 1024)
    fac = jnp.where(q_pos < seq_len, a_own / length, 0.0)
    st_fin[pl.ds(0, 8), :] = fac
    st_fin[pl.ds(8, 8), :] = dsum

    def masked(b, c):
        own = b * 2 + core
        oth = b * 2 + 1 - core
        rows = pl.ds(m(b * 128, 128), 128)
        at_own[rows, :] = (o_t[col(own), :] * st_fin[pl.ds(own, 1), :]).astype(BF)
        at_oth[rows, :] = (o_t[col(oth), :] * st_fin[pl.ds(oth, 1), :]).astype(BF)
        return c

    lax.fori_loop(0, 4, masked, 0)

    def weighted(at, r, ys):
        return dot_nn(at[pl.ds(m(r * 256, 256), 256), :], gb[:, pl.ds(m(ys * 768, 128), 768)]) * weight

    for d in (2, 1, 3, 0):
        ys = ys_of(d)

        def away(r, c):
            gw_send[d, pl.ds(m(r * 256, 256), 256), :] = weighted(at_oth, r, ys).astype(BF)
            return c

        lax.fori_loop(0, 2, away, 0)
        sends.append(send(gw_send.at[d], gw_got.at[d], s_gc.at[d], r_gc.at[d], other))

    def backward(h, c):
        for t in range(4):
            cols = pl.ds(t * QT, QT)
            dp = dot_nn(vb[:, col(h)], do_t[col(h), cols])
            f = st_fin[pl.ds(h, 1), cols]
            ds[:, cols] = (pn[h, :, cols].astype(F32) * f * (dp - st_fin[pl.ds(8 + h, 1), cols])).astype(BF)
        scaled = (do_t[col(h), :].astype(F32) * st_fin[pl.ds(h, 1), :]).astype(BF)
        dv_fin[:, col(h)] = dot_nt(pn[h], scaled).astype(BF)
        dk_fin[:, col(h)] = (dot_nn(ds[...], qb[:, col(h)]) * SCALE).astype(BF)
        mine = dot_nn(kt[col(h), :], ds[:, pl.ds(own0, 512)]) * SCALE
        away = dot_nn(kt[col(h), :], ds[:, pl.ds(oth0, 512)]) * SCALE
        dq_own[:, col(h)] = mine.T
        dq_send[:, col(h)] = away.T.astype(BF)
        return c

    outs = ((dq_fin, dq_out), (dk_fin, dk_out), (dv_fin, dv_out))

    def out_cols(b, xs):
        return pl.ds(m((b * 4 + xs) * 256, 256), 256)

    def give(a, b):
        src, dst = outs[a]
        for d in (1, 3, 2):
            xp = xs_of(d)
            sends.append(send(
                src.at[pl.ds(m(xp * 128, 128), 128), pl.ds(b * 256, 256)], dst.at[:, out_cols(b, x)],
                s_out.at[a, b, d], r_out.at[a, b, x], dev(x_=xp)))
        local(src.at[pl.ds(m(x * 128, 128), 128), pl.ds(b * 256, 256)], dst.at[:, out_cols(b, x)],
              14 + a * 4 + b)

    def finish(b):
        cols = pl.ds(b * 256, 256)
        got(dq_got.at[:, cols], r_dq.at[b])
        dq_fin[:, cols] = (dq_own[:, cols] + dq_got[:, cols].astype(F32)).astype(BF)
        give(0, b)

    def fold(d):
        ys = ys_of(d)
        got(gw_got.at[d], r_gc.at[d])

        def mine(r, c):
            rows = pl.ds(m(r * 256, 256), 256)
            gy_send[d, rows, :] = (weighted(at_own, r, ys) + gw_got[d, rows, :].astype(F32)).astype(BF)
            return c

        lax.fori_loop(0, 2, mine, 0)
        if d:
            sends.append(send(gy_send.at[d], gy_got.at[d], s_gy.at[d], r_gy.at[d], dev(y_=ys_of(d))))

    for b in range(4):
        lax.fori_loop(b * 2, b * 2 + 2, backward, 0)
        sends.append(send(
            dq_send.at[:, pl.ds(b * 256, 256)], dq_got.at[:, pl.ds(b * 256, 256)],
            s_dq.at[b], r_dq.at[b], mate))
        give(1, b)
        give(2, b)
        if b == 0:
            for d in (2, 1, 3, 0):
                fold(d)
        else:
            finish(b - 1)

    for d in (1, 3, 2):
        got(gy_got.at[d], r_gy.at[d])

    def gather_y(r, c):
        rows = pl.ds(m(r * 128, 128), 128)
        t = gy_send[0, rows, :].astype(F32)
        for d in (1, 2, 3):
            t = t + gy_got[d, rows, :].astype(F32)
        gz[rows, :] = t.astype(BF)
        return c

    lax.fori_loop(0, 4, gather_y, 0)

    def gz_blk(zz):
        return gz.at[pl.ds(m(lax.div(zz, 2) * 128, 128), 128), pl.ds(m(lax.rem(zz, 2) * 384, 128), 384)]

    for d in (4, 3, 5, 2, 6, 1, 7):
        zz = zs_of(d)
        sends.append(send(gz_blk(zz), gz_got.at[d], s_gzz.at[d], r_gzz.at[d], zdev(zz)))

    finish(3)

    for d in range(1, 8):
        got(gz_got.at[d], r_gzz.at[d])
    t = gz_blk(z)[...].astype(F32)
    for d in range(1, 8):
        t = t + gz_got[d].astype(F32)
    rolled = pltpu.roll(t, 192, 1)
    fin_send[...] = jnp.where(core == 0, rolled, t)[:, :192]
    sends.append(send(fin_send, fin_got, s_fin.at[0], s_fin.at[1], other))
    gw_out[pl.ds(m(core * 128, 128), 128), :] = jnp.where(core == 0, t, rolled)[:, :192]

    for b in range(4):
        for a in range(3):
            for d in (1, 3, 2):
                xs = xs_of(d)
                got(outs[a][1].at[:, out_cols(b, xs)], r_out.at[a, b, xs])
    got(fin_got, s_fin.at[1])
    gw_out[pl.ds(m((1 - core) * 128, 128), 128), :] = fin_got[...]

    for c in sends:
        c.wait_send()
    for a in range(3):
        for d in (1, 2, 3):
            got(q_rows(half, x), s_qkv.at[a * 4 + d])
    for c in loc[14:]:
        c.wait()


def shards(*args):
    any_ = pl.BlockSpec(memory_space=pl.ANY)
    smem = pl.BlockSpec(memory_space=pltpu.SMEM)
    tok = jax.ShapeDtypeStruct((128, 4096), BF)
    dma = pltpu.SemaphoreType.DMA
    return pl.pallas_call(
        kernel,
        out_shape=(tok, tok, tok, jax.ShapeDtypeStruct((256, 192), F32)),
        in_specs=[smem] * 3 + [any_] * 5,
        out_specs=(any_, any_, any_, pl.BlockSpec(memory_space=pltpu.VMEM)),
        scratch_shapes=[
            pltpu.VMEM((1024, 1024), BF), pltpu.VMEM((512, 1024), BF), pltpu.VMEM((512, 1024), BF),
            pltpu.VMEM((1024, 512), BF), pltpu.VMEM((1024, 512), BF),
            pltpu.VMEM((1024, 3072), BF), pltpu.VMEM((1024, 3072), BF),
            pltpu.VMEM((1024, 1024), BF), pltpu.VMEM((8, 512, 1024), BF), pltpu.VMEM((1024, 1024), F32),
            pltpu.VMEM((512, 1024), BF), pltpu.VMEM((512, 1024), BF),
            pltpu.VMEM((128, 192), BF), pltpu.VMEM((128, 192), BF), pltpu.VMEM((512, QT), F32),
            pltpu.VMEM((24, 1024), F32), pltpu.VMEM((24, 1024), F32), pltpu.VMEM((16, 1024), F32),
            pltpu.VMEM((512, 1024), BF),
            pltpu.VMEM((512, 1024), F32), pltpu.VMEM((512, 1024), BF), pltpu.VMEM((512, 1024), BF),
            pltpu.VMEM((512, 1024), BF), pltpu.VMEM((512, 1024), BF), pltpu.VMEM((512, 1024), BF),
            pltpu.VMEM((4, 512, 768), BF), pltpu.VMEM((4, 512, 768), BF),
            pltpu.VMEM((4, 512, 768), BF), pltpu.VMEM((4, 512, 768), BF),
            pltpu.VMEM((512, 768), BF), pltpu.VMEM((8, 128, 384), BF),
            pltpu.VMEM((128, 192), F32), pltpu.VMEM((128, 192), F32),
            dma((26,)), dma((12,)), dma((3, 4)), dma((4,)), dma((4,)), dma((4,)), dma((4,)),
            dma((24,)), dma((2, 4, 4)), dma((40,)), dma, dma((8,)), dma((4, 4)), dma((4, 4)),
            dma((2,)), dma((4,)), dma((4,)), dma((3, 4, 4)), dma((3, 4, 4)), dma((4,)), dma((4,)),
            dma((4,)), dma((4,)), dma((8,)), dma((8,)), dma((2,)),
        ],
        compiler_params=pltpu.CompilerParams(
            collective_id=0, has_side_effects=True, vmem_limit_bytes=67043328
        ),
    )(*args)


def solution(mesh):
    row = P(("grp", "sp"), None)
    return jax.shard_map(
        shards, mesh=mesh,
        in_specs=(P(), P(), P(), row, row, row, row, P("sp", "grp")),
        out_specs=(row, row, row, P("sp", "grp")),
        check_vma=False,
    )
```

```python
import jax
import jax.numpy as jnp
from jax import lax
from jax.experimental import pallas as pl
from jax.experimental.pallas import tpu as pltpu
from jax.sharding import PartitionSpec as P

MESH = pl.DeviceIdType.MESH
BF = jnp.bfloat16
F32 = jnp.float32
LOG2E = 1.4426950408889634
SCALE = 128 ** (-0.5)
NEG = -1e30
QT = 256


def dot_nn(a, b):
    return lax.dot_general(a, b, (((1,), (0,)), ((), ())), preferred_element_type=F32)


def dot_nt(a, b):
    return lax.dot_general(a, b, (((1,), (1,)), ((), ())), preferred_element_type=F32)


def dot_tn(a, b):
    return lax.dot_general(a, b, (((0,), (0,)), ((), ())), preferred_element_type=F32)


def kernel(
    bucket_ref, len_ref, cnt_ref, q_in, k_in, v_in, g_in, w_in,
    dq_out, dk_out, dv_out, gw_out,
    qb, kb, vb, kt, vt, gb, wb, do_t, pn, o_t, at,
    w_own, w_got, bias, st_own, st_got, st_fin, ds,
    dq_own, dq_send, dq_got, dq_fin, dk_fin, dv_fin,
    gw_send, gw_got, gy_send, gy_got, gz, gl_got, gz2, gz_got, fin, fin_got,
    s_loc, s_qkv, r_qkv, s_q2, r_q2, s_gz, r_gz, s_gx, r_gx, s_w, r_wc, r_wz, r_wl, r_wy, r_wd,
    s_st, r_st, s_dq, r_dq, s_out, r_out, s_gc, r_gc, s_gy, r_gy, s_gl, r_gl, s_g2, r_g2, s_fin,
):
    g = lax.axis_index("grp")
    s = lax.axis_index("sp")
    core = lax.rem(g, 2)
    zl = lax.rem(lax.div(g, 2), 2)
    y = lax.div(g, 4)
    x = lax.rem(s, 4)
    zh = lax.div(s, 4)
    half = lax.rem(zh, 2)
    pair = lax.div(zh, 2)

    def dev(x_=None, zh_=None, y_=None, zl_=None, core_=None):
        x_ = x if x_ is None else x_
        zh_ = zh if zh_ is None else zh_
        y_ = y if y_ is None else y_
        zl_ = zl if zl_ is None else zl_
        core_ = core if core_ is None else core_
        return {"grp": y_ * 4 + zl_ * 2 + core_, "sp": zh_ * 4 + x_}

    def xs_of(d):
        return lax.rem(x + d, 4)

    def ys_of(d):
        return lax.rem(y + d, 4)

    other = dev(core_=1 - core)
    mate_zh = zh + 1 - 2 * half
    mate = dev(zh_=mate_zh)
    zmate = dev(zl_=1 - zl)

    def m(v, k):
        return pl.multiple_of(v, k)

    sends = []

    def send(src, dst, ss, rs, device):
        c = pltpu.make_async_remote_copy(
            src_ref=src, dst_ref=dst, send_sem=ss, recv_sem=rs, device_id=device, device_id_type=MESH
        )
        c.start()
        return c

    def got(ref, sem):
        pltpu.make_async_copy(ref, ref, sem).wait()

    open_scope = []

    def mark(name):
        if open_scope:
            open_scope.pop().__exit__(None, None, None)
        if name:
            open_scope.append(jax.named_scope(name))
            open_scope[-1].__enter__()

    mark("barrier")
    barrier = pltpu.get_barrier_semaphore()
    peers = [dev(x_=xs_of(d)) for d in (1, 2, 3)]
    peers += [dev(y_=ys_of(d)) for d in (1, 2, 3)]
    peers += [dev(zh_=lax.rem(zh + d, 4)) for d in (1, 2, 3)]
    peers += [other, zmate]
    for p in peers:
        pl.semaphore_signal(barrier, inc=1, device_id=p, device_id_type=MESH)
    pl.semaphore_wait(barrier, len(peers))

    seq_len = len_ref[bucket_ref[g]]
    total = cnt_ref[bucket_ref[0]]
    for i in range(1, 16):
        total = total + cnt_ref[bucket_ref[i]]
    weight = cnt_ref[bucket_ref[g]].astype(F32) / total.astype(F32)

    row_me = half * 512 + x * 128
    loc = []

    def local(src, dst, i):
        c = pltpu.make_async_copy(src, dst, s_loc.at[i])
        c.start()
        loc.append(c)
        return c

    mark("first")

    def blocks(src, dst, row, xp):
        out = []
        for b in range(4):
            out.append((src.at[:, pl.ds(m((b * 4 + xp) * 256, 256), 256)],
                        dst.at[pl.ds(row, 128), pl.ds(b * 256, 256)]))
        return out

    arrs = ((q_in, qb, m(row_me, 128)), (k_in, kb, m(x * 128, 128)), (v_in, vb, m(x * 128, 128)))

    def send_x(a):
        src, dst, row = arrs[a]
        for d in (1, 3, 2):
            xp = xs_of(d)
            for sr, dr in blocks(src, dst, row, xp):
                send(sr, dr, s_qkv.at[a * 4 + d], r_qkv.at[a, x], dev(x_=xp))

    sends.append(send(
        w_in.at[:, pl.ds(m((1 - core) * 128, 128), 128)], w_got, s_w.at[0], r_wc, other))
    lw = local(w_in.at[:, pl.ds(m(core * 128, 128), 128)], w_own, 0)
    for a in range(3):
        send_x(a)
    for a in range(3):
        src, dst, row = arrs[a]
        for b, (sr, dr) in enumerate(blocks(src, dst, row, x)):
            local(sr, dr, 1 + a * 4 + b)
    local(g_in, gb.at[pl.ds(m(row_me, 128), 128), :], 13)

    mark("w_core")
    r_i = lax.broadcasted_iota(jnp.int32, (192, 384), 0)
    c_i = lax.broadcasted_iota(jnp.int32, (192, 384), 1)
    e_own = jnp.where(c_i == r_i + core * 192, 1.0, 0.0).astype(BF)
    e_oth = jnp.where(c_i == r_i + (1 - core) * 192, 1.0, 0.0).astype(BF)
    lw.wait()
    got(w_got, r_wc)

    def w_blk(zh_, zl_):
        return wb.at[pl.ds(m(zh_ * 256 + core * 128, 128), 128), pl.ds(m((y * 2 + zl_) * 384, 128), 384)]

    w_blk(zh, zl)[...] = (dot_tn(w_own[...], e_own) + dot_tn(w_got[...], e_oth)).astype(BF)
    for d in (2, 1, 3):
        sends.append(send(
            w_blk(zh, zl), w_blk(zh, zl), s_w.at[d], r_wz.at[zh], dev(zh_=lax.rem(zh + d, 4))))

    def g_mate(i):
        sends.append(send(
            g_in.at[pl.ds(i * 32, 32), :], gb.at[pl.ds(m(row_me + i * 32, 32), 32), :],
            s_gz.at[i], r_gz.at[i], mate))

    left, right = dev(x_=xs_of(3)), dev(x_=xs_of(1))
    xl, xr = xs_of(3), xs_of(1)
    oh = 1 - half

    def g_rows(hh, xs, i):
        return gb.at[pl.ds(m(hh * 512 + xs * 128 + i * 32, 32), 32), :]

    g_mate(0)
    for i in (0, 2, 1, 3):
        for j, p in enumerate((right, left)):
            sends.append(send(
                g_in.at[pl.ds(i * 32, 32), :], g_rows(half, x, i),
                s_gx.at[i * 2 + j], r_gx.at[0, x, i], p))
    mark("w_z_wait")
    for d in (1, 3, 2):
        zs = lax.rem(zh + d, 4)
        got(w_blk(zs, zl), r_wz.at[zs])
    for b in range(4):
        sends.append(send(w_blk(b, zl), w_blk(b, zl), s_w.at[4 + b], r_wl.at[b], zmate))
    for i in (1, 2, 3):
        g_mate(i)

    mark("w_l_wait")

    def w_row(ys, b):
        return wb.at[pl.ds(m(b * 256 + core * 128, 128), 128), pl.ds(m(ys * 768, 128), 768)]

    for b in range(4):
        got(w_blk(b, 1 - zl), r_wl.at[b])
        for d in (2, 1, 3):
            sends.append(send(
                w_row(y, b), w_row(y, b), s_w.at[8 + b * 4 + d], r_wy.at[y, b], dev(y_=ys_of(d))))
        sends.append(send(w_row(y, b), w_row(y, b), s_w.at[8 + b * 4], r_wd.at[y, b], other))

    mark("q_relay")
    for c in loc[1:5]:
        c.wait()

    def bt_of(t):
        return lax.rem(t + 2 * (1 - pair), 4)

    def q_rows(hh, xs):
        return qb.at[pl.ds(m(hh * 512 + xs * 128, 128), 128), :]

    for d in (1, 3, 2):
        got(q_rows(half, xs_of(d)), r_qkv.at[0, xs_of(d)])
    own0 = m(half * 512, 512)
    oth0 = m((1 - half) * 512, 512)

    def q_blk(r0, t):
        return qb.at[pl.ds(r0, 512), pl.ds(m(bt_of(t) * 256, 256), 256)]

    for t in range(4):
        sends.append(send(q_blk(own0, t), q_blk(own0, t), s_q2.at[t], r_q2.at[t], mate))

    def relay(hh, k, i, sem):
        src, to = (xr, left) if i < 2 else (xl, right)
        got(g_rows(hh, src, i), r_gx.at[k, src, i])
        sends.append(send(g_rows(hh, src, i), g_rows(hh, src, i), s_gx.at[sem + i], r_gx.at[k, src, i], to))

    mark("kv_wait")
    for c in loc[5:]:
        c.wait()
    n_loc = len(loc)
    for a, buf in ((1, kb), (2, vb)):
        for d in (1, 3, 2):
            xs = xs_of(d)
            got(buf.at[pl.ds(m(xs * 128, 128), 128), :], r_qkv.at[a, xs])

    mark("flip")
    key_pos = lax.broadcasted_iota(jnp.int32, (512, QT), 0) + half * 512
    bias[...] = jnp.where(key_pos < seq_len, 0.0, NEG)

    def col(h):
        return pl.ds(m(h * 128, 128), 128)

    def flip(h, c):
        kt[col(h), :] = kb[:, col(h)].T
        vt[col(h), :] = vb[:, col(h)].T
        return c

    lax.fori_loop(0, 8, flip, 0)

    def forward(t, first, r0):
        def body(n, c):
            j = lax.rem(n, 2)
            tt = t + lax.div(n, 4)
            h = bt_of(tt) * 2 + j
            q0 = m(r0 + lax.rem(lax.div(n, 2), 2) * QT, QT)
            sc = dot_nt(kb[:, col(h)], qb[pl.ds(q0, QT), col(h)])
            sc = sc * (SCALE * LOG2E) + bias[...]
            top = jnp.max(sc, axis=0, keepdims=True)
            pe = jnp.exp2(sc - top)
            st_own[tt, pl.ds(j, 1), pl.ds(q0, QT)] = top
            st_own[tt, pl.ds(2 + j, 1), pl.ds(q0, QT)] = jnp.sum(pe, axis=0, keepdims=True)
            pb = pe.astype(BF)
            pn[h, :, pl.ds(q0, QT)] = pb
            o_t[col(h), pl.ds(q0, QT)] = dot_nn(vt[col(h), :], pb)
            return c

        lax.fori_loop(0, first, body, 0)

    mark("fwd_own")
    forward(0, 16, own0)

    for i in (0, 1, 2, 3):
        mark(f"g_mate_{i}")
        got(g_rows(oh, x, i), r_gz.at[i])
        for j, p in enumerate((right, left)):
            sends.append(send(
                g_rows(oh, x, i), g_rows(oh, x, i), s_gx.at[12 + i * 2 + j], r_gx.at[1, x, i], p))
    for i in (0, 2, 1, 3):
        mark(f"g_relay_{i}")
        relay(half, 0, i, 8)

    mark("w_y_wait")
    for d in (1, 3, 2):
        ys = ys_of(d)
        for b in range(4):
            got(w_row(ys, b), r_wy.at[ys, b])
            sends.append(send(w_row(ys, b), w_row(ys, b), s_w.at[24 + d * 4 + b], r_wd.at[ys, b], other))

    def w_row_oth(ys, b):
        return wb.at[pl.ds(m(b * 256 + (1 - core) * 128, 128), 128), pl.ds(m(ys * 768, 128), 768)]

    def g_rest(hh, k):
        for i in range(4):
            got(g_rows(hh, xl if i < 2 else xr, i), r_gx.at[k, xl if i < 2 else xr, i])
            got(g_rows(hh, xs_of(2), i), r_gx.at[k, xs_of(2), i])

    def grads(q0):
        def body(i, c):
            rows = pl.ds(m(i * 256, 256), 256)
            do_t[rows, pl.ds(q0, 256)] = dot_nt(wb[rows, :], gb[pl.ds(q0, 256), :]).astype(BF)
            return c

        lax.fori_loop(0, 4, body, 0)

    mark("g_own_wait")
    g_rest(half, 0)
    for i in (0, 2):
        mark(f"g_relay2_{i}")
        relay(oh, 1, i, 20)
    mark("w_d2d_wait")
    for d in range(4):
        ys = ys_of(d)
        for b in range(4):
            got(w_row_oth(ys, b), r_wd.at[ys, b])
    mark("grads_own0")
    grads(own0)
    for i in (1, 3):
        mark(f"g_relay2_{i}")
        relay(oh, 1, i, 20)
    mark("grads_own1")
    grads(m(own0 + 256, 256))

    q_pos = lax.broadcasted_iota(jnp.int32, (2, 1024), 1)

    def weighted(ys):
        return dot_nn(at[...], gb[:, pl.ds(m(ys * 768, 128), 768)]) * weight

    outs = ((dq_fin, dq_out), (dk_fin, dk_out), (dv_fin, dv_out))

    def out_cols(b, xs):
        return pl.ds(m((b * 4 + xs) * 256, 256), 256)

    def give(a, t):
        b = bt_of(t)
        src, dst = outs[a]
        for d in (1, 3, 2):
            xp = xs_of(d)
            sends.append(send(
                src.at[pl.ds(m(xp * 128, 128), 128), pl.ds(m(b * 256, 256), 256)], dst.at[:, out_cols(b, x)],
                s_out.at[a, t, d], r_out.at[a, t, x], dev(x_=xp)))
        local(src.at[pl.ds(m(x * 128, 128), 128), pl.ds(m(b * 256, 256), 256)], dst.at[:, out_cols(b, x)],
              14 + a * 4 + t)

    def finish(t):
        mark(f"finish_{t}")
        cols = pl.ds(m(bt_of(t) * 256, 256), 256)
        got(dq_got.at[:, cols], r_dq.at[t])
        dq_fin[:, cols] = (dq_own[:, cols] + dq_got[:, cols].astype(F32)).astype(BF)
        give(0, t)

    def fold(t):
        mark(f"fold_{t}")
        got(gw_got.at[t], r_gc.at[t])
        for d in (2, 1, 3, 0):
            gy_send[t, d] = (gy_send[t, d].astype(F32) + gw_got[t, d].astype(F32)).astype(BF)
            if d:
                sends.append(send(
                    gy_send.at[t, d], gy_got.at[t, d], s_gy.at[t, d], r_gy.at[t, d], dev(y_=ys_of(d))))

    def gather_y(t):
        mark(f"gather_y_{t}")
        for d in (1, 3, 2):
            got(gy_got.at[t, d], r_gy.at[t, d])
        v = gy_send[t, 0].astype(F32)
        for d in (1, 2, 3):
            v = v + gy_got[t, d].astype(F32)
        gz[t, 0] = v[:, :384].astype(BF)
        gz[t, 1] = v[:, 384:].astype(BF)
        sends.append(send(gz.at[t, 1 - zl], gl_got.at[t], s_gl.at[t], r_gl.at[t], zmate))

    def fold_l(t):
        mark(f"fold_l_{t}")
        got(gl_got.at[t], r_gl.at[t])
        gz2[t] = (gz[t, zl].astype(F32) + gl_got[t].astype(F32)).astype(BF)
        if t < 2:
            sends.append(send(gz2.at[t], gz_got.at[half], s_g2.at[t], r_g2.at[half], dev(zh_=bt_of(t))))

    def query(t):
        mark(f"q_wait_{t}")
        got(q_blk(oth0, t), r_q2.at[t])
        mark(f"fwd_{t}")
        forward(t, 4, oth0)

    def stats(t):
        mark(f"grads_oth_{t}")
        bt = bt_of(t)
        rows = pl.ds(m(bt * 256, 256), 256)
        for u in range(2):
            q0 = m(oth0 + u * 256, 256)
            do_t[rows, pl.ds(q0, 256)] = dot_nt(wb[rows, :], gb[pl.ds(q0, 256), :]).astype(BF)
        for j in range(2):
            h = bt * 2 + j
            st_own[t, pl.ds(4 + j, 1), :] = jnp.sum(
                do_t[col(h), :].astype(F32) * o_t[col(h), :], axis=0, keepdims=True)
        sends.append(send(st_own.at[t], st_got.at[t], s_st.at[t], r_st.at[t], mate))

    def merge(t):
        mark(f"st_wait_{t}")
        got(st_got.at[t], r_st.at[t])
        top_own, top_got = st_own[t, 0:2, :], st_got[t, 0:2, :]
        top = jnp.maximum(top_own, top_got)
        a_own, a_got = jnp.exp2(top_own - top), jnp.exp2(top_got - top)
        length = st_own[t, 2:4, :] * a_own + st_got[t, 2:4, :] * a_got
        st_fin[t, 2:4, :] = (st_own[t, 4:6, :] * a_own + st_got[t, 4:6, :] * a_got) / length
        st_fin[t, 0:2, :] = jnp.where(q_pos < seq_len, a_own / length, 0.0)

    def back(t):
        mark(f"back_{t}")
        bt = bt_of(t)
        cols = pl.ds(m(bt * 256, 256), 256)

        def backward(j, c):
            h = bt * 2 + j
            for u in range(4):
                cu = pl.ds(u * QT, QT)
                dp = dot_nn(vb[:, col(h)], do_t[col(h), cu])
                f = st_fin[t, pl.ds(j, 1), cu]
                ds[:, cu] = (pn[h, :, cu].astype(F32) * f * (dp - st_fin[t, pl.ds(2 + j, 1), cu])).astype(BF)
            scaled = (do_t[col(h), :].astype(F32) * st_fin[t, pl.ds(j, 1), :]).astype(BF)
            away = dot_nn(kt[col(h), :], ds[:, pl.ds(oth0, 512)]) * SCALE
            dq_send[:, col(h)] = away.T.astype(BF)
            mine = dot_nn(kt[col(h), :], ds[:, pl.ds(own0, 512)]) * SCALE
            dq_own[:, col(h)] = mine.T
            dv_fin[:, col(h)] = dot_nt(pn[h], scaled).astype(BF)
            dk_fin[:, col(h)] = (dot_nn(ds[...], qb[:, col(h)]) * SCALE).astype(BF)
            return c

        lax.fori_loop(0, 2, backward, 0)
        sends.append(send(dq_send.at[:, cols], dq_got.at[:, cols], s_dq.at[t], r_dq.at[t], mate))
        give(1, t)
        give(2, t)

    def gw(t):
        mark(f"gw_{t}")
        bt = bt_of(t)
        at[0:128, :] = (o_t[col(bt * 2 + core), :] * st_fin[t, pl.ds(core, 1), :]).astype(BF)
        at[128:256, :] = (o_t[col(bt * 2 + 1 - core), :] * st_fin[t, pl.ds(1 - core, 1), :]).astype(BF)

        def gw_part(d, c):
            r = weighted(lax.rem(y + d, 4))
            gy_send[t, d] = r[:128].astype(BF)
            gw_send[t, d] = r[128:].astype(BF)
            return c

        lax.fori_loop(0, 4, gw_part, 0)
        sends.append(send(gw_send.at[t], gw_got.at[t], s_gc.at[t], r_gc.at[t], other))

    query(0)
    query(1)
    mark("g_oth_wait")
    g_rest(oh, 1)
    stats(0)
    stats(1)
    merge(0)
    back(0)
    gw(0)
    query(2)
    stats(2)
    merge(1)
    back(1)
    fold(0)
    gw(1)
    query(3)
    stats(3)
    merge(2)
    gw(2)
    back(2)
    fold(1)
    gather_y(0)
    finish(0)
    merge(3)
    gw(3)
    fold(2)
    back(3)
    gather_y(1)
    fold_l(0)
    fold(3)
    finish(1)
    gather_y(2)
    fold_l(1)
    gather_y(3)
    fold_l(2)
    finish(2)
    fold_l(3)
    sends.append(send(gz2.at[3 - half], gz_got.at[2], s_g2.at[2], r_g2.at[2], mate))
    finish(3)

    mark("gz_wait")
    for d in range(3):
        got(gz_got.at[d], r_g2.at[d])
    mark("gz_sum")
    v = gz2[2 + half].astype(F32)
    for d in range(3):
        v = v + gz_got[d].astype(F32)
    fin[...] = v.T
    sends.append(send(
        fin.at[pl.ds(m((1 - core) * 192, 64), 192), :], fin_got, s_fin.at[0], s_fin.at[1], other))
    gw_out[:, pl.ds(m(core * 128, 128), 128)] = fin[pl.ds(m(core * 192, 64), 192), :]

    mark("out_wait")
    for t in range(4):
        for a in (1, 2, 0):
            for d in (1, 3, 2):
                xs = xs_of(d)
                got(outs[a][1].at[:, out_cols(bt_of(t), xs)], r_out.at[a, t, xs])
    mark("fin_wait")
    got(fin_got, s_fin.at[1])
    gw_out[:, pl.ds(m((1 - core) * 128, 128), 128)] = fin_got[...]

    mark("send_wait")
    for c in sends:
        c.wait_send()
    for a in range(3):
        for d in (1, 2, 3):
            got(q_rows(half, x), s_qkv.at[a * 4 + d])
    for c in loc[n_loc:]:
        c.wait()
    mark(None)


def shards(*args):
    any_ = pl.BlockSpec(memory_space=pl.ANY)
    smem = pl.BlockSpec(memory_space=pltpu.SMEM)
    tok = jax.ShapeDtypeStruct((128, 4096), BF)
    dma = pltpu.SemaphoreType.DMA
    vm = pltpu.VMEM
    dq, dk, dv, gw = pl.pallas_call(
        kernel,
        out_shape=(tok, tok, tok, jax.ShapeDtypeStruct((192, 256), F32)),
        in_specs=[smem] * 3 + [any_] * 5,
        out_specs=(any_, any_, any_, pl.BlockSpec(memory_space=pltpu.VMEM)),
        scratch_shapes=[
            vm((1024, 1024), BF), vm((512, 1024), BF), vm((512, 1024), BF),
            vm((1024, 512), BF), vm((1024, 512), BF),
            vm((1024, 3072), BF), vm((1024, 3072), BF),
            vm((1024, 1024), BF), vm((8, 512, 1024), BF), vm((1024, 1024), F32),
            vm((256, 1024), BF),
            vm((192, 128), BF), vm((192, 128), BF), vm((512, QT), F32),
            vm((4, 8, 1024), F32), vm((4, 8, 1024), F32), vm((4, 8, 1024), F32),
            vm((512, 1024), BF),
            vm((512, 1024), F32), vm((512, 1024), BF), vm((512, 1024), BF),
            vm((512, 1024), BF), vm((512, 1024), BF), vm((512, 1024), BF),
            vm((4, 4, 128, 768), BF), vm((4, 4, 128, 768), BF),
            vm((4, 4, 128, 768), BF), vm((4, 4, 128, 768), BF),
            vm((4, 2, 128, 384), BF), vm((4, 128, 384), BF), vm((4, 128, 384), BF), vm((3, 128, 384), BF),
            vm((384, 128), F32), vm((192, 128), F32),
            dma((26,)), dma((12,)), dma((3, 4)), dma((4,)), dma((4,)), dma((4,)), dma((4,)),
            dma((24,)), dma((2, 4, 4)), dma((40,)), dma, dma((4,)), dma((4,)), dma((4, 4)), dma((4, 4)),
            dma((4,)), dma((4,)), dma((4,)), dma((4,)), dma((3, 4, 4)), dma((3, 4, 4)),
            dma((4,)), dma((4,)), dma((4, 4)), dma((4, 4)), dma((4,)), dma((4,)), dma((3,)), dma((3,)), dma((2,)),
        ],
        compiler_params=pltpu.CompilerParams(
            collective_id=0, has_side_effects=True, vmem_limit_bytes=67043328
        ),
    )(*args[:7], args[7].T)
    return dq, dk, dv, gw.T


def solution(mesh):
    row = P(("grp", "sp"), None)
    return jax.shard_map(
        shards, mesh=mesh,
        in_specs=(P(), P(), P(), row, row, row, row, P("sp", "grp")),
        out_specs=(row, row, row, P("sp", "grp")),
        check_vma=False,
    )
```

```python
import jax
import jax.numpy as jnp
from jax import lax
from jax.experimental import pallas as pl
from jax.experimental.pallas import tpu as pltpu
from jax.sharding import PartitionSpec as P

MESH = pl.DeviceIdType.MESH
BF = jnp.bfloat16
F32 = jnp.float32
LOG2E = 1.4426950408889634
SCALE = 128 ** (-0.5)
NEG = -1e30
QT = 256


def dot_nn(a, b):
    return lax.dot_general(a, b, (((1,), (0,)), ((), ())), preferred_element_type=F32)


def dot_nt(a, b):
    return lax.dot_general(a, b, (((1,), (1,)), ((), ())), preferred_element_type=F32)


def dot_tn(a, b):
    return lax.dot_general(a, b, (((0,), (0,)), ((), ())), preferred_element_type=F32)


def kernel(
    bucket_ref, len_ref, cnt_ref, q_in, k_in, v_in, g_in, w_in,
    dq_out, dk_out, dv_out, gw_out,
    qb, kb, vb, kt, vt, gb, wb, do_t, pn, o_t, at,
    w_own, w_got, bias, st_own, st_got, st_fin, ds,
    dq_own, dq_send, dq_got, dq_fin, dk_fin, dv_fin,
    gw_send, gw_got, gy_send, gy_got, gz, gl_got, gz2, gz_got, fin, fin_got,
    s_loc, s_qkv, r_qkv, s_q2, r_q2, s_gz, r_gz, s_gx, r_gx, s_w, r_wc, r_wz, r_wl, r_wy, r_wd,
    s_st, r_st, s_dq, r_dq, s_out, r_out, s_gc, r_gc, s_gy, r_gy, s_gl, r_gl, s_g2, r_g2, s_fin,
):
    g = lax.axis_index("grp")
    s = lax.axis_index("sp")
    core = lax.rem(g, 2)
    zl = lax.rem(lax.div(g, 2), 2)
    y = lax.div(g, 4)
    x = lax.rem(s, 4)
    zh = lax.div(s, 4)
    half = lax.rem(zh, 2)
    pair = lax.div(zh, 2)

    def dev(x_=None, zh_=None, y_=None, zl_=None, core_=None):
        x_ = x if x_ is None else x_
        zh_ = zh if zh_ is None else zh_
        y_ = y if y_ is None else y_
        zl_ = zl if zl_ is None else zl_
        core_ = core if core_ is None else core_
        return {"grp": y_ * 4 + zl_ * 2 + core_, "sp": zh_ * 4 + x_}

    def xs_of(d):
        return lax.rem(x + d, 4)

    def ys_of(d):
        return lax.rem(y + d, 4)

    other = dev(core_=1 - core)
    mate_zh = zh + 1 - 2 * half
    mate = dev(zh_=mate_zh)
    zmate = dev(zl_=1 - zl)
    free_zh = lax.rem(zh + 3 + 2 * half, 4)
    free = dev(zh_=free_zh)

    def bt_of(t):
        return lax.rem(t + 2 * (1 - pair), 4)

    def m(v, k):
        return pl.multiple_of(v, k)

    sends = []

    def send(src, dst, ss, rs, device):
        c = pltpu.make_async_remote_copy(
            src_ref=src, dst_ref=dst, send_sem=ss, recv_sem=rs, device_id=device, device_id_type=MESH
        )
        c.start()
        return c

    def got(ref, sem):
        pltpu.make_async_copy(ref, ref, sem).wait()

    open_scope = []

    def mark(name):
        if open_scope:
            open_scope.pop().__exit__(None, None, None)
        if name:
            open_scope.append(jax.named_scope(name))
            open_scope[-1].__enter__()

    mark("barrier")
    barrier = pltpu.get_barrier_semaphore()
    peers = [dev(x_=xs_of(d)) for d in (1, 2, 3)]
    peers += [dev(y_=ys_of(d)) for d in (1, 2, 3)]
    peers += [mate, free, other, zmate]
    for p in peers:
        pl.semaphore_signal(barrier, inc=1, device_id=p, device_id_type=MESH)
    pl.semaphore_wait(barrier, len(peers))

    seq_len = len_ref[bucket_ref[g]]
    total = cnt_ref[bucket_ref[0]]
    for i in range(1, 16):
        total = total + cnt_ref[bucket_ref[i]]
    weight = cnt_ref[bucket_ref[g]].astype(F32) / total.astype(F32)

    row_me = half * 512 + x * 128
    loc = []

    def local(src, dst, i):
        c = pltpu.make_async_copy(src, dst, s_loc.at[i])
        c.start()
        loc.append(c)
        return c

    mark("first")

    def blocks(src, dst, row, xp, steps):
        out = []
        for t in steps:
            b = bt_of(t)
            out.append((src.at[:, pl.ds(m((b * 4 + xp) * 256, 256), 256)],
                        dst.at[pl.ds(row, 128), pl.ds(m(b * 256, 256), 256)]))
        return out

    arrs = ((q_in, qb, m(row_me, 128)), (k_in, kb, m(x * 128, 128)), (v_in, vb, m(x * 128, 128)))

    def send_x(a, k, steps):
        src, dst, row = arrs[a]
        for d in (1, 3, 2):
            xp = xs_of(d)
            for sr, dr in blocks(src, dst, row, xp, steps):
                send(sr, dr, s_qkv.at[(a * 2 + k) * 4 + d], r_qkv.at[a, k, x], dev(x_=xp))

    sends.append(send(
        w_in.at[:, pl.ds(m((1 - core) * 128, 128), 128)], w_got, s_w.at[0], r_wc, other))
    lw = local(w_in.at[:, pl.ds(m(core * 128, 128), 128)], w_own, 0)
    send_x(0, 0, (0, 1, 2, 3))
    send_x(1, 0, (0, 1))
    send_x(2, 0, (0, 1))
    for a in range(3):
        src, dst, row = arrs[a]
        for b, (sr, dr) in enumerate(blocks(src, dst, row, x, (0, 1, 2, 3))):
            local(sr, dr, 1 + a * 4 + b)
    local(g_in, gb.at[pl.ds(m(row_me, 128), 128), :], 13)

    mark("w_core")
    r_i = lax.broadcasted_iota(jnp.int32, (192, 384), 0)
    c_i = lax.broadcasted_iota(jnp.int32, (192, 384), 1)
    e_own = jnp.where(c_i == r_i + core * 192, 1.0, 0.0).astype(BF)
    e_oth = jnp.where(c_i == r_i + (1 - core) * 192, 1.0, 0.0).astype(BF)
    lw.wait()
    got(w_got, r_wc)

    def w_blk(zh_, zl_):
        return wb.at[pl.ds(m(zh_ * 256 + core * 128, 128), 128), pl.ds(m((y * 2 + zl_) * 384, 128), 384)]

    w_blk(zh, zl)[...] = (dot_tn(w_own[...], e_own) + dot_tn(w_got[...], e_oth)).astype(BF)
    sends.append(send(w_blk(zh, zl), w_blk(zh, zl), s_w.at[1], r_wz.at[zh], mate))
    sends.append(send(w_blk(zh, zl), w_blk(zh, zl), s_w.at[2], r_wz.at[zh], free))

    def g_mate(i):
        sends.append(send(
            g_in.at[pl.ds(i * 32, 32), :], gb.at[pl.ds(m(row_me + i * 32, 32), 32), :],
            s_gz.at[i], r_gz.at[i], mate))

    left, right = dev(x_=xs_of(3)), dev(x_=xs_of(1))
    xl, xr = xs_of(3), xs_of(1)
    oh = 1 - half

    def g_rows(hh, xs, i):
        return gb.at[pl.ds(m(hh * 512 + xs * 128 + i * 32, 32), 32), :]

    g_mate(0)
    for i in (0, 2, 1, 3):
        for j, p in enumerate((right, left)):
            sends.append(send(
                g_in.at[pl.ds(i * 32, 32), :], g_rows(half, x, i),
                s_gx.at[i * 2 + j], r_gx.at[0, x, i], p))
    mark("w_z_wait")
    got(w_blk(mate_zh, zl), r_wz.at[mate_zh])
    sends.append(send(w_blk(mate_zh, zl), w_blk(mate_zh, zl), s_w.at[3], r_wz.at[mate_zh], free))
    for zs in (free_zh, lax.rem(zh + 2, 4)):
        got(w_blk(zs, zl), r_wz.at[zs])
    for b in range(4):
        sends.append(send(w_blk(b, zl), w_blk(b, zl), s_w.at[4 + b], r_wl.at[b], zmate))
    for i in (1, 2, 3):
        g_mate(i)

    mark("w_l_wait")

    def w_row(ys, b):
        return wb.at[pl.ds(m(b * 256 + core * 128, 128), 128), pl.ds(m(ys * 768, 128), 768)]

    for b in range(4):
        got(w_blk(b, 1 - zl), r_wl.at[b])
        for d in (2, 1, 3):
            sends.append(send(
                w_row(y, b), w_row(y, b), s_w.at[8 + b * 4 + d], r_wy.at[y, b], dev(y_=ys_of(d))))
        sends.append(send(w_row(y, b), w_row(y, b), s_w.at[8 + b * 4], r_wd.at[y, b], other))

    mark("q_relay")
    for c in loc[1:5]:
        c.wait()

    def q_rows(hh, xs):
        return qb.at[pl.ds(m(hh * 512 + xs * 128, 128), 128), :]

    for d in (1, 3, 2):
        got(q_rows(half, xs_of(d)), r_qkv.at[0, 0, xs_of(d)])
    own0 = m(half * 512, 512)
    oth0 = m((1 - half) * 512, 512)

    def q_blk(r0, t):
        return qb.at[pl.ds(r0, 512), pl.ds(m(bt_of(t) * 256, 256), 256)]

    def q_send(t):
        sends.append(send(q_blk(own0, t), q_blk(own0, t), s_q2.at[t], r_q2.at[t], mate))

    q_send(0)
    q_send(1)

    def relay(hh, k, i, sem):
        src, to = (xr, left) if i < 2 else (xl, right)
        got(g_rows(hh, src, i), r_gx.at[k, src, i])
        sends.append(send(g_rows(hh, src, i), g_rows(hh, src, i), s_gx.at[sem + i], r_gx.at[k, src, i], to))

    mark("kv_wait")
    for c in loc[5:]:
        c.wait()
    n_loc = len(loc)

    def kv_wait(k):
        for a, buf in ((1, kb), (2, vb)):
            for d in (1, 3, 2):
                xs = xs_of(d)
                got(buf.at[pl.ds(m(xs * 128, 128), 128), pl.ds(m(bt_of(2 * k) * 256, 256), 512)], r_qkv.at[a, k, xs])

    kv_wait(0)

    mark("flip")
    key_pos = lax.broadcasted_iota(jnp.int32, (512, QT), 0) + half * 512
    bias[...] = jnp.where(key_pos < seq_len, 0.0, NEG)

    def col(h):
        return pl.ds(m(h * 128, 128), 128)

    def flip(n, c):
        h = bt_of(lax.div(n, 2)) * 2 + lax.rem(n, 2)
        kt[col(h), :] = kb[:, col(h)].T
        vt[col(h), :] = vb[:, col(h)].T
        return c

    lax.fori_loop(0, 4, flip, 0)

    def forward(t, first, r0):
        def body(n, c):
            j = lax.rem(n, 2)
            tt = t + lax.div(n, 4)
            h = bt_of(tt) * 2 + j
            q0 = m(r0 + lax.rem(lax.div(n, 2), 2) * QT, QT)
            sc = dot_nt(kb[:, col(h)], qb[pl.ds(q0, QT), col(h)])
            sc = sc * (SCALE * LOG2E) + bias[...]
            top = jnp.max(sc, axis=0, keepdims=True)
            pe = jnp.exp2(sc - top)
            st_own[tt, pl.ds(j, 1), pl.ds(q0, QT)] = top
            st_own[tt, pl.ds(2 + j, 1), pl.ds(q0, QT)] = jnp.sum(pe, axis=0, keepdims=True)
            pb = pe.astype(BF)
            pn[h, :, pl.ds(q0, QT)] = pb
            o_t[col(h), pl.ds(q0, QT)] = dot_nn(vt[col(h), :], pb)
            return c

        lax.fori_loop(0, first, body, 0)

    def query(t):
        mark(f"q_wait_{t}")
        got(q_blk(oth0, t), r_q2.at[t])
        mark(f"fwd_{t}")
        forward(t, 4, oth0)

    mark("fwd_own")
    forward(0, 8, own0)

    def from_mate(i):
        mark(f"g_mate_{i}")
        got(g_rows(oh, x, i), r_gz.at[i])
        for j, p in enumerate((right, left)):
            sends.append(send(
                g_rows(oh, x, i), g_rows(oh, x, i), s_gx.at[12 + i * 2 + j], r_gx.at[1, x, i], p))

    def own_relay(i):
        mark(f"g_relay_{i}")
        relay(half, 0, i, 8)

    own_relay(0)
    own_relay(2)
    from_mate(0)
    from_mate(1)
    own_relay(1)
    own_relay(3)
    from_mate(2)
    from_mate(3)

    mark("w_y_wait")
    for d in (1, 3, 2):
        ys = ys_of(d)
        for b in range(4):
            got(w_row(ys, b), r_wy.at[ys, b])
            sends.append(send(w_row(ys, b), w_row(ys, b), s_w.at[24 + d * 4 + b], r_wd.at[ys, b], other))

    def w_row_oth(ys, b):
        return wb.at[pl.ds(m(b * 256 + (1 - core) * 128, 128), 128), pl.ds(m(ys * 768, 128), 768)]

    def g_rest(hh, k):
        for i in range(4):
            got(g_rows(hh, xl if i < 2 else xr, i), r_gx.at[k, xl if i < 2 else xr, i])
            got(g_rows(hh, xs_of(2), i), r_gx.at[k, xs_of(2), i])

    def grads(q0):
        def body(i, c):
            rows = pl.ds(m(i * 256, 256), 256)
            do_t[rows, pl.ds(q0, 256)] = dot_nt(wb[rows, :], gb[pl.ds(q0, 256), :]).astype(BF)
            return c

        lax.fori_loop(0, 4, body, 0)

    q_send(2)
    query(0)
    mark("g_own_wait")
    g_rest(half, 0)
    for i in (0, 2):
        mark(f"g_relay2_{i}")
        relay(oh, 1, i, 20)
    mark("w_d2d_wait")
    for d in range(4):
        ys = ys_of(d)
        for b in range(4):
            got(w_row_oth(ys, b), r_wd.at[ys, b])
    mark("grads_own0")
    grads(own0)
    for i in (1, 3):
        mark(f"g_relay2_{i}")
        relay(oh, 1, i, 20)
    for a in (1, 2):
        send_x(a, 1, (2, 3))
    mark("grads_own1")
    grads(m(own0 + 256, 256))

    q_pos = lax.broadcasted_iota(jnp.int32, (2, 1024), 1)

    def weighted(ys):
        return dot_nn(at[...], gb[:, pl.ds(m(ys * 768, 128), 768)]) * weight

    outs = ((dq_fin, dq_out), (dk_fin, dk_out), (dv_fin, dv_out))

    def out_cols(b, xs):
        return pl.ds(m((b * 4 + xs) * 256, 256), 256)

    def give(a, t):
        b = bt_of(t)
        src, dst = outs[a]
        for d in (1, 3, 2):
            xp = xs_of(d)
            sends.append(send(
                src.at[pl.ds(m(xp * 128, 128), 128), pl.ds(m(b * 256, 256), 256)], dst.at[:, out_cols(b, x)],
                s_out.at[a, t, d], r_out.at[a, t, x], dev(x_=xp)))
        local(src.at[pl.ds(m(x * 128, 128), 128), pl.ds(m(b * 256, 256), 256)], dst.at[:, out_cols(b, x)],
              14 + a * 4 + t)

    def finish(t):
        mark(f"finish_{t}")
        cols = pl.ds(m(bt_of(t) * 256, 256), 256)
        got(dq_got.at[:, cols], r_dq.at[t])
        dq_fin[:, cols] = (dq_own[:, cols] + dq_got[:, cols].astype(F32)).astype(BF)
        give(0, t)

    def fold(t):
        mark(f"fold_{t}")
        got(gw_got.at[t], r_gc.at[t])
        for d in (2, 1, 3, 0):
            gy_send[t, d] = (gy_send[t, d].astype(F32) + gw_got[t, d].astype(F32)).astype(BF)
            if d:
                sends.append(send(
                    gy_send.at[t, d], gy_got.at[t, d], s_gy.at[t, d], r_gy.at[t, d], dev(y_=ys_of(d))))

    def gather_y(t):
        mark(f"gather_y_{t}")
        for d in (1, 3, 2):
            got(gy_got.at[t, d], r_gy.at[t, d])
        v = gy_send[t, 0].astype(F32)
        for d in (1, 2, 3):
            v = v + gy_got[t, d].astype(F32)
        gz[t, 0] = v[:, :384].astype(BF)
        gz[t, 1] = v[:, 384:].astype(BF)
        sends.append(send(gz.at[t, 1 - zl], gl_got.at[t], s_gl.at[t], r_gl.at[t], zmate))

    def fold_l(t):
        mark(f"fold_l_{t}")
        got(gl_got.at[t], r_gl.at[t])
        gz2[t] = (gz[t, zl].astype(F32) + gl_got[t].astype(F32)).astype(BF)
        if t < 2:
            sends.append(send(
                gz2.at[t], gz_got.at[lax.rem(t + half, 2)], s_g2.at[t], r_g2.at[lax.rem(t + half, 2)], free))

    def stats(t):
        mark(f"grads_oth_{t}")
        bt = bt_of(t)
        rows = pl.ds(m(bt * 256, 256), 256)
        for u in range(2):
            q0 = m(oth0 + u * 256, 256)
            do_t[rows, pl.ds(q0, 256)] = dot_nt(wb[rows, :], gb[pl.ds(q0, 256), :]).astype(BF)
        for j in range(2):
            h = bt * 2 + j
            st_own[t, pl.ds(4 + j, 1), :] = jnp.sum(
                do_t[col(h), :].astype(F32) * o_t[col(h), :], axis=0, keepdims=True)
        sends.append(send(st_own.at[t], st_got.at[t], s_st.at[t], r_st.at[t], mate))

    def merge(t):
        mark(f"st_wait_{t}")
        got(st_got.at[t], r_st.at[t])
        top_own, top_got = st_own[t, 0:2, :], st_got[t, 0:2, :]
        top = jnp.maximum(top_own, top_got)
        a_own, a_got = jnp.exp2(top_own - top), jnp.exp2(top_got - top)
        length = st_own[t, 2:4, :] * a_own + st_got[t, 2:4, :] * a_got
        st_fin[t, 2:4, :] = (st_own[t, 4:6, :] * a_own + st_got[t, 4:6, :] * a_got) / length
        st_fin[t, 0:2, :] = jnp.where(q_pos < seq_len, a_own / length, 0.0)

    def back(t):
        mark(f"back_{t}")
        bt = bt_of(t)
        cols = pl.ds(m(bt * 256, 256), 256)

        def backward(j, c):
            h = bt * 2 + j
            for u in range(4):
                cu = pl.ds(u * QT, QT)
                dp = dot_nn(vb[:, col(h)], do_t[col(h), cu])
                f = st_fin[t, pl.ds(j, 1), cu]
                ds[:, cu] = (pn[h, :, cu].astype(F32) * f * (dp - st_fin[t, pl.ds(2 + j, 1), cu])).astype(BF)
            scaled = (do_t[col(h), :].astype(F32) * st_fin[t, pl.ds(j, 1), :]).astype(BF)
            away = dot_nn(kt[col(h), :], ds[:, pl.ds(oth0, 512)]) * SCALE
            dq_send[:, col(h)] = away.T.astype(BF)
            mine = dot_nn(kt[col(h), :], ds[:, pl.ds(own0, 512)]) * SCALE
            dq_own[:, col(h)] = mine.T
            dv_fin[:, col(h)] = dot_nt(pn[h], scaled).astype(BF)
            dk_fin[:, col(h)] = (dot_nn(ds[...], qb[:, col(h)]) * SCALE).astype(BF)
            return c

        lax.fori_loop(0, 2, backward, 0)
        sends.append(send(dq_send.at[:, cols], dq_got.at[:, cols], s_dq.at[t], r_dq.at[t], mate))
        give(1, t)
        give(2, t)

    def gw(t):
        mark(f"gw_{t}")
        bt = bt_of(t)
        at[0:128, :] = (o_t[col(bt * 2 + core), :] * st_fin[t, pl.ds(core, 1), :]).astype(BF)
        at[128:256, :] = (o_t[col(bt * 2 + 1 - core), :] * st_fin[t, pl.ds(1 - core, 1), :]).astype(BF)

        def gw_part(d, c):
            r = weighted(lax.rem(y + d, 4))
            gy_send[t, d] = r[:128].astype(BF)
            gw_send[t, d] = r[128:].astype(BF)
            return c

        lax.fori_loop(0, 4, gw_part, 0)
        sends.append(send(gw_send.at[t], gw_got.at[t], s_gc.at[t], r_gc.at[t], other))

    query(1)
    mark("g_oth_wait")
    g_rest(oh, 1)
    stats(0)
    stats(1)
    q_send(3)
    merge(0)
    back(0)
    gw(0)
    mark("kv_wait2")
    kv_wait(1)
    mark("flip2")
    lax.fori_loop(4, 8, flip, 0)
    mark("fwd_own_2")
    forward(2, 4, own0)
    query(2)
    stats(2)
    merge(1)
    back(1)
    fold(0)
    gw(1)
    mark("fwd_own_3")
    forward(3, 4, own0)
    query(3)
    stats(3)
    fold(1)
    merge(2)
    gw(2)
    back(2)
    fold(2)
    gather_y(0)
    finish(0)
    merge(3)
    gw(3)
    gather_y(1)
    fold(3)
    back(3)
    finish(1)
    gather_y(2)
    fold_l(0)
    fold_l(1)
    finish(2)
    gather_y(3)
    finish(3)
    fold_l(2)
    fold_l(3)
    mark("g_free_wait")
    got(gz_got.at[0], r_g2.at[0])
    gz2[3 - half] = (gz2[3 - half].astype(F32) + gz_got[0].astype(F32)).astype(BF)
    sends.append(send(gz2.at[3 - half], gz_got.at[2], s_g2.at[2], r_g2.at[2], mate))

    mark("gz_wait")
    for d in (1, 2):
        got(gz_got.at[d], r_g2.at[d])
    mark("gz_sum")
    v = gz2[2 + half].astype(F32)
    for d in (1, 2):
        v = v + gz_got[d].astype(F32)
    fin[...] = v.T
    sends.append(send(
        fin.at[pl.ds(m((1 - core) * 192, 64), 192), :], fin_got, s_fin.at[0], s_fin.at[1], other))
    gw_out[:, pl.ds(m(core * 128, 128), 128)] = fin[pl.ds(m(core * 192, 64), 192), :]

    mark("out_wait")
    for t in range(4):
        for a in (1, 2, 0):
            for d in (1, 3, 2):
                xs = xs_of(d)
                got(outs[a][1].at[:, out_cols(bt_of(t), xs)], r_out.at[a, t, xs])
    mark("fin_wait")
    got(fin_got, s_fin.at[1])
    gw_out[:, pl.ds(m((1 - core) * 128, 128), 128)] = fin_got[...]

    mark("send_wait")
    for c in sends:
        c.wait_send()
    for d in (1, 2, 3):
        got(q_rows(half, x), s_qkv.at[d])
        for a in (1, 2):
            for k in (0, 1):
                got(kb.at[pl.ds(0, 128), pl.ds(0, 512)], s_qkv.at[(a * 2 + k) * 4 + d])
    for c in loc[n_loc:]:
        c.wait()
    mark(None)


def store(a, b, c, d, ao, bo, co, do, sem):
    copies = [pltpu.make_async_copy(p, o, sem.at[i]) for i, (p, o) in enumerate(((a, ao), (b, bo), (c, co), (d, do)))]
    for c in copies:
        c.start()
    for c in copies:
        c.wait()


def shards(*args):
    any_ = pl.BlockSpec(memory_space=pl.ANY)
    smem = pl.BlockSpec(memory_space=pltpu.SMEM)
    vmem = pl.BlockSpec(memory_space=pltpu.VMEM)
    tok = pltpu.VMEM((128, 4096), BF)
    dma = pltpu.SemaphoreType.DMA
    vm = pltpu.VMEM
    parts = pl.pallas_call(
        kernel,
        out_shape=(tok, tok, tok, pltpu.VMEM((192, 256), F32)),
        in_specs=[smem] * 3 + [any_] * 5,
        out_specs=(vmem,) * 4,
        scratch_shapes=[
            vm((1024, 1024), BF), vm((512, 1024), BF), vm((512, 1024), BF),
            vm((1024, 512), BF), vm((1024, 512), BF),
            vm((1024, 3072), BF), vm((1024, 3072), BF),
            vm((1024, 1024), BF), vm((8, 512, 1024), BF), vm((1024, 1024), F32),
            vm((256, 1024), BF),
            vm((192, 128), BF), vm((192, 128), BF), vm((512, QT), F32),
            vm((4, 8, 1024), F32), vm((4, 8, 1024), F32), vm((4, 8, 1024), F32),
            vm((512, 1024), BF),
            vm((512, 1024), F32), vm((512, 1024), BF), vm((512, 1024), BF),
            vm((512, 1024), BF), vm((512, 1024), BF), vm((512, 1024), BF),
            vm((4, 4, 128, 768), BF), vm((4, 4, 128, 768), BF),
            vm((4, 4, 128, 768), BF), vm((4, 4, 128, 768), BF),
            vm((4, 2, 128, 384), BF), vm((4, 128, 384), BF), vm((4, 128, 384), BF), vm((3, 128, 384), BF),
            vm((384, 128), F32), vm((192, 128), F32),
            dma((26,)), dma((24,)), dma((3, 2, 4)), dma((4,)), dma((4,)), dma((4,)), dma((4,)),
            dma((24,)), dma((2, 4, 4)), dma((40,)), dma, dma((4,)), dma((4,)), dma((4, 4)), dma((4, 4)),
            dma((4,)), dma((4,)), dma((4,)), dma((4,)), dma((3, 4, 4)), dma((3, 4, 4)),
            dma((4,)), dma((4,)), dma((4, 4)), dma((4, 4)), dma((4,)), dma((4,)), dma((3,)), dma((3,)), dma((2,)),
        ],
        compiler_params=pltpu.CompilerParams(
            collective_id=0, has_side_effects=True, vmem_limit_bytes=59768832
        ),
    )(*args[:7], args[7].T)
    hbm = jax.ShapeDtypeStruct((128, 4096), BF)
    dq, dk, dv, gw = pl.pallas_call(
        store,
        out_shape=(hbm, hbm, hbm, jax.ShapeDtypeStruct((192, 256), F32)),
        in_specs=[vmem] * 4,
        out_specs=(any_,) * 4,
        scratch_shapes=[dma((4,))],
        compiler_params=pltpu.CompilerParams(vmem_limit_bytes=4194304),
    )(*parts)
    return dq, dk, dv, gw.T


def solution(mesh):
    row = P(("grp", "sp"), None)
    return jax.shard_map(
        shards, mesh=mesh,
        in_specs=(P(), P(), P(), row, row, row, row, P("sp", "grp")),
        out_specs=(row, row, row, P("sp", "grp")),
        check_vma=False,
    )
```
